16 devices in a mesh: dp: 4 (over y, z, core), sp: 4 (over x).
Axes of the slice: x: 4, y: 2, z: 1, core: 2. Of those that a mesh axis runs over, the one named last changes fastest.
The devices are a block of a 4x4x8 slice.
Arguments:
- x: bfloat16 [8192, 7168], P(('dp', 'sp')), parts along dimension 0
- gain: bfloat16 [7168], replicated
- wq: bfloat16 [7168, 7168], replicated
- wk: bfloat16 [7168, 7168], replicated
- wv: bfloat16 [7168, 7168], replicated
- wo: bfloat16 [7168, 7168], replicated
Outputs:
- output: bfloat16 [8192, 7168], P(('dp', 'sp')), parts along dimension 0
There are 4 independent parts. The reference program is written for one: setup_inputs(seed, part) draws one part's arguments, and reference() takes and returns one part's arrays. A program takes and returns all parts, laid end to end along the dimension named above; an argument that names none is the same for every part.
All inputs are finite; a program needn't handle non-finite values.
Results may differ from the reference program's by a relative error of at most 0.012.
Values are sent between devices in bfloat16 or wider.
A program may use at most 768 MiB of HBM per device.

```python
import jax
import jax.numpy as jnp
from jax import lax

ROWS = 2048
D = 7168
HEADS = 56
KV_HEADS = 56
HEAD = 128
THETA = 10000


def setup_inputs(seed: int = 0, part: int = 0) -> dict:
    kx, kn, kq, kk, kv, ko = jax.random.split(jax.random.key(seed), 6)

    def weights(key, rows, columns):
        return jax.random.normal(key, (rows, columns), jnp.float32) * rows**-0.5

    drawn = {
        "x": jax.random.normal(jax.random.fold_in(kx, part), (ROWS, D), jnp.float32),
        "gain": 1 + 0.1 * jax.random.normal(kn, (D,), jnp.float32),
        "wq": 2 * weights(kq, D, HEADS * HEAD),
        "wk": 2 * weights(kk, D, KV_HEADS * HEAD),
        "wv": 4 * weights(kv, D, KV_HEADS * HEAD),
        "wo": weights(ko, HEADS * HEAD, D),
    }
    return {k: v.astype(jnp.bfloat16) for k, v in drawn.items()}


def normed(x, gain):
    wide = x.astype(jnp.float32)
    scale = lax.rsqrt(jnp.mean(wide * wide, -1, keepdims=True) + 1e-6)
    return (wide * scale * gain.astype(jnp.float32)).astype(jnp.bfloat16)


def turned(t, place, theta):
    half = t.shape[-1] // 2
    angle = place.astype(jnp.float32)[:, None] * theta ** (-jnp.arange(half, dtype=jnp.float32) / half)
    cos, sin = jnp.cos(angle)[:, None], jnp.sin(angle)[:, None]
    a, b = t[..., :half].astype(jnp.float32), t[..., half:].astype(jnp.float32)
    return jnp.concatenate([a * cos - b * sin, b * cos + a * sin], -1).astype(jnp.bfloat16)


def matmul(a, w):
    return jnp.dot(a, w, preferred_element_type=jnp.float32).astype(jnp.bfloat16)


def einsum(form, a, b):
    return jnp.einsum(form, a.astype(jnp.float32), b.astype(jnp.float32))


def attention(q, k, v):
    scores = einsum("tgsd,ugd->gstu", q, k) * q.shape[-1] ** -0.5
    token = jnp.arange(q.shape[0])
    scores = jnp.where(token[:, None] >= token, scores, -jnp.inf)
    weights = jax.nn.softmax(scores, -1).astype(jnp.bfloat16)
    return einsum("gstu,ugd->tgsd", weights, v).astype(jnp.bfloat16)


def reference(x, gain, wq, wk, wv, wo):
    a, place = normed(x, gain), jnp.arange(ROWS)
    q = turned(matmul(a, wq).reshape(ROWS, HEADS, HEAD), place, THETA).reshape(ROWS, KV_HEADS, -1, HEAD)
    k = turned(matmul(a, wk).reshape(ROWS, KV_HEADS, HEAD), place, THETA)
    v = matmul(a, wv).reshape(ROWS, KV_HEADS, HEAD)
    seen = attention(q, k, v).reshape(ROWS, HEADS * HEAD)
    return (x.astype(jnp.float32) + jnp.dot(seen, wo, preferred_element_type=jnp.float32)).astype(jnp.bfloat16)
```

```python
import functools

import jax
import jax.numpy as jnp
from jax import lax
from jax.experimental import pallas as pl
from jax.experimental.pallas import tpu as pltpu
from jax.sharding import PartitionSpec as P

HEAD = 128
THETA = 10000
LOG2E = 1.4426950408889634
MESH = pl.DeviceIdType.MESH
PER = 2
TILE = 512
SLOTS = 12
HIDDEN = -1e30


def _dot(a, b, ca, cb):
    return lax.dot_general(a, b, (((ca,), (cb,)), ((), ())), preferred_element_type=jnp.float32)


def _kernel(n, x_hbm, gain_ref, cos_ref, sin_ref, wq, wk, wv, wo, y_hbm, qkv_hbm, o_hbm,
            a, w, acc, raw, out, qkv, vt, o, xt, asem, wsem, csend, crecv, lsem, dsend, drecv, xsem, ysem):
    me = lax.axis_index("sp")
    dp = lax.axis_index("dp")
    own, width = a.shape
    part = PER * HEAD
    span = n * part
    rounds = width // span
    ntile = width // TILE
    per_round = 3 * (span // TILE)
    homes = TILE // part
    tiles = rounds * per_round
    groups = [(0, rounds - 2), (rounds - 2, rounds - 1), (rounds - 1, rounds)]

    barrier = pltpu.get_barrier_semaphore()
    for s in range(1, n):
        pl.semaphore_signal(barrier, inc=1, device_id=(dp, lax.rem(me + s, n)), device_id_type=MESH)

    def w_copy(ref, i, slot):
        return pltpu.make_async_copy(ref.at[:, pl.ds(pl.multiple_of(i * TILE, TILE), TILE)], w.at[slot], wsem.at[slot])

    def w_start(i):
        for t, ref in enumerate((wk, wv, wq)):
            @pl.when(lax.rem(i, 3) == t)
            def _():
                w_copy(ref, lax.div(i, 3), lax.rem(i, 2)).start()

    def wo_copy(g, j):
        lo, hi = groups[g][0] * span, groups[g][1] * span
        slot = lax.rem(j, 2)
        return pltpu.make_async_copy(wo.at[pl.ds(lo, hi - lo), pl.ds(pl.multiple_of(j * TILE, TILE), TILE)],
                                     w.at[slot, pl.ds(0, hi - lo)], wsem.at[slot])

    w_start(jnp.int32(0))
    w_start(jnp.int32(1))
    strip = 16
    load = pltpu.make_async_copy(x_hbm, a, asem.at[0])
    load.start()
    raw[1] = jnp.zeros_like(raw[1])
    load.wait()

    def norm(i, _):
        rows = pl.ds(pl.multiple_of(i * strip, strip), strip)
        sums = jnp.zeros((strip, 128), jnp.float32)
        for c in range(0, width, 512):
            v = a[rows, c : c + 512].astype(jnp.float32)
            v = v * v
            sums = sums + ((v[:, :128] + v[:, 128:256]) + (v[:, 256:384] + v[:, 384:]))
        scale = lax.rsqrt(jnp.sum(sums, -1, keepdims=True) / width + 1e-6)
        for c in range(0, width, 512):
            v = a[rows, c : c + 512].astype(jnp.float32)
            a[rows, c : c + 512] = (v * scale * gain_ref[:, c : c + 512].astype(jnp.float32)).astype(jnp.bfloat16)
        return 0

    lax.fori_loop(0, own // strip, norm, 0)
    pl.semaphore_wait(barrier, n - 1)

    def tile_of(i):
        return lax.div(i, per_round), lax.rem(i, 3), lax.rem(lax.div(i, 3), span // TILE) * homes

    def c_copy(i, e):
        r, t, home = tile_of(i)
        slot = lax.rem(i, SLOTS)
        return pltpu.make_async_remote_copy(out.at[slot, e], qkv_hbm.at[r, me, t], csend.at[slot, e], crecv.at[r, me],
                                            device_id=(dp, home + e), device_id_type=MESH)

    def c_own(i, e):
        r, t, home = tile_of(i)
        return pltpu.make_async_copy(out.at[lax.rem(i, SLOTS), e], qkv_hbm.at[r, me, t], crecv.at[r, me])

    def c_send(i):
        for e in range(homes):
            @pl.when(tile_of(i)[2] + e != me)
            def _():
                c_copy(i, e).start()

            @pl.when(tile_of(i)[2] + e == me)
            def _():
                c_own(i, e).start()

    def c_sent(i):
        for e in range(homes):
            @pl.when(tile_of(i)[2] + e != me)
            def _():
                c_copy(i, e).wait_send()

    def turn(i):
        t = lax.rem(i, 3)
        kind = lax.select(t == 1, 1, 0)
        slot = lax.rem(i, SLOTS)
        for c in range(TILE // HEAD):
            v = raw[lax.rem(i, 2), :, c * HEAD : (c + 1) * HEAD].astype(jnp.float32)
            v = v * cos_ref[kind] + pltpu.roll(v, HEAD // 2, 1) * sin_ref[kind]
            e, at = c // PER, c % PER * HEAD
            out[slot, e, :, at : at + HEAD] = v.astype(jnp.bfloat16)

    def project(i):
        w_copy(wq, 0, lax.rem(i, 2)).wait()

        @pl.when(i > SLOTS)
        def _():
            c_sent(i - 1 - SLOTS)

        before = lax.rem(i + tiles * SLOTS - 1, tiles * SLOTS)
        raw[lax.rem(i, 2)] = jnp.dot(a[...], w[lax.rem(i, 2)], preferred_element_type=jnp.float32).astype(jnp.bfloat16)
        turn(before)

        @pl.when(i > 0)
        def _():
            c_send(i - 1)

        @pl.when(i + 2 < tiles)
        def _():
            w_start(i + 2)

        @pl.when(i + 2 >= tiles)
        def _():
            wo_copy(0, i + 2 - tiles).start()

    e2 = HEAD**-0.5 * LOG2E

    def d_copy(r, b):
        slot = lax.rem(r, 2)
        to = o_hbm.at[:, pl.ds(pl.multiple_of(r * span + me * part, part), part)]
        return pltpu.make_async_remote_copy(o.at[slot, b], to, dsend.at[slot, b], drecv.at[r, me],
                                            device_id=(dp, b), device_id_type=MESH)

    def d_own(r, b):
        to = o_hbm.at[:, pl.ds(pl.multiple_of(r * span + me * part, part), part)]
        return pltpu.make_async_copy(o.at[lax.rem(r, 2), b], to, drecv.at[r, me])

    def d_sent(r):
        for b in range(n):
            @pl.when(b != me)
            def _():
                d_copy(r, b).wait_send()

    def attend(r):
        loads = []
        for s in range(n):
            pltpu.make_async_copy(qkv_hbm.at[r, s], qkv_hbm.at[r, s], crecv.at[r, s]).wait()
            loads.append(pltpu.make_async_copy(qkv_hbm.at[r, s], qkv.at[s], lsem.at[s]))
            loads[-1].start()

        @pl.when(r >= 1)
        def _():
            d_own(r - 1, me).wait()

        @pl.when(r >= 2)
        def _():
            d_sent(r - 2)

        for load in loads:
            load.wait()
        slot = lax.rem(r, 2)
        ok = lax.broadcasted_iota(jnp.int32, (own, own), 0) <= lax.broadcasted_iota(jnp.int32, (own, own), 1)
        for h in range(PER):
            for j in range(n):
                vt[h, j] = qkv[j, 1, :, h * HEAD : (h + 1) * HEAD].T
        pieces = [(h, i) for i in range(n) for h in range(PER)]

        def scores(h, i):
            q = qkv[i, 2, :, h * HEAD : (h + 1) * HEAD]
            s = [_dot(qkv[j, 0, :, h * HEAD : (h + 1) * HEAD], q, 1, 1) for j in range(i + 1)]
            s[i] = jnp.where(ok, s[i], HIDDEN)
            return s

        ahead = scores(*pieces[0])
        for k, (h, i) in enumerate(pieces):
            s = ahead
            if k + 1 < len(pieces):
                ahead = scores(*pieces[k + 1])
            top = functools.reduce(jnp.maximum, [t.max(axis=0, keepdims=True) for t in s]) * e2
            total, mix = 0.0, 0.0
            for j, t in enumerate(s):
                p = jnp.exp2(t * e2 - top)
                total = total + p.sum(axis=0, keepdims=True)
                mix = mix + _dot(vt[h, j], p.astype(jnp.bfloat16), 1, 0)
            o[slot, i, :, h * HEAD : (h + 1) * HEAD] = (mix * (1 / total)).T.astype(jnp.bfloat16)
        for b in range(n):
            @pl.when(b != me)
            def _():
                d_copy(r, b).start()

            @pl.when(b == me)
            def _():
                d_own(r, b).start()

    def x_copy(j):
        slot = lax.rem(j, 2)
        return pltpu.make_async_copy(x_hbm.at[:, pl.ds(pl.multiple_of(j * TILE, TILE), TILE)], xt.at[slot], xsem.at[slot])

    def y_copy(j):
        slot = lax.rem(j, 2)
        return pltpu.make_async_copy(raw.at[slot], y_hbm.at[:, pl.ds(pl.multiple_of(j * TILE, TILE), TILE)], ysem.at[slot])

    def combine(g):
        lo, hi = groups[g][0] * span, groups[g][1] * span
        for r in range(*groups[g]):
            for s in range(n):
                @pl.when(s != me)
                def _():
                    at = o_hbm.at[:, pl.ds(r * span + s * part, part)]
                    pltpu.make_async_copy(at, at, drecv.at[r, s]).wait()
        if g == len(groups) - 1:
            d_own(rounds - 1, me).wait()
        load = pltpu.make_async_copy(o_hbm.at[:, pl.ds(lo, hi - lo)], a.at[:, pl.ds(lo, hi - lo)], asem.at[0])
        load.start()
        last = g == len(groups) - 1
        if last:
            x_copy(0).start()
            x_copy(1).start()
        load.wait()

        def body(j, _):
            slot = lax.rem(j, 2)
            wo_copy(g, j).wait()
            if last:
                x_copy(j).wait()

                @pl.when(j >= 2)
                def _():
                    y_copy(j - 2).wait()
            got = jnp.dot(a[:, lo:hi], w[slot, : hi - lo], preferred_element_type=jnp.float32)
            if g:
                got = got + acc[j]
            if last:
                raw[slot] = (xt[slot].astype(jnp.float32) + got).astype(jnp.bfloat16)
                y_copy(j).start()
            else:
                acc[j] = got

            @pl.when(j + 2 < ntile)
            def _():
                wo_copy(g, j + 2).start()
                if last:
                    x_copy(j + 2).start()
            if not last:
                @pl.when(j + 2 >= ntile)
                def _():
                    wo_copy(g + 1, j + 2 - ntile).start()
            return 0

        lax.fori_loop(0, ntile, body, 0)
        if last:
            y_copy(ntile - 2).wait()
            y_copy(ntile - 1).wait()

    def step(r, _):
        @pl.when(r < rounds)
        def _():
            def one(k, _):
                project(r * per_round + k)
                return 0

            lax.fori_loop(0, per_round, one, 0)

        @pl.when(r == rounds - 1)
        def _():
            c_sent(jnp.int32(tiles - 1 - SLOTS))
            turn(jnp.int32(tiles - 1))
            c_send(jnp.int32(tiles - 1))

        @pl.when(r == rounds)
        def _():
            combine(0)

        @pl.when(r > 0)
        def _():
            attend(r - 1)

        return 0

    lax.fori_loop(0, rounds + 1, step, 0)
    combine(1)
    combine(2)
    for i in range(tiles - SLOTS, tiles):
        c_sent(jnp.int32(i))
    d_sent(rounds - 2)
    d_sent(rounds - 1)


def solution(mesh):
    n = mesh.shape["sp"]

    def step(x, gain, wq, wk, wv, wo):
        own, width = x.shape
        part = PER * HEAD
        rounds = width // (n * part)
        place = lax.axis_index("sp") * own + jnp.arange(own)
        half = HEAD // 2
        angle = place.astype(jnp.float32)[:, None] * THETA ** (-jnp.arange(half, dtype=jnp.float32) / half)
        cos, sin = jnp.cos(angle), jnp.sin(angle)
        one = jnp.ones((own, HEAD), jnp.float32)
        cos = jnp.stack([jnp.concatenate([cos, cos], -1), one])
        sin = jnp.stack([jnp.concatenate([-sin, sin], -1), 0 * one])
        anywhere, vmem = pl.BlockSpec(memory_space=pl.ANY), pl.BlockSpec(memory_space=pltpu.VMEM)
        y, _, _ = pl.pallas_call(
            functools.partial(_kernel, n),
            out_shape=[jax.ShapeDtypeStruct((own, width), jnp.bfloat16),
                       jax.ShapeDtypeStruct((rounds, n, 3, own, part), jnp.bfloat16),
                       jax.ShapeDtypeStruct((own, width), jnp.bfloat16)],
            in_specs=[anywhere, vmem, vmem, vmem] + [anywhere] * 4,
            out_specs=[anywhere] * 3,
            scratch_shapes=[
                pltpu.VMEM((own, width), jnp.bfloat16),
                pltpu.VMEM((2, width, TILE), jnp.bfloat16),
                pltpu.VMEM((width // TILE, own, TILE), jnp.float32),
                pltpu.VMEM((2, own, TILE), jnp.bfloat16),
                pltpu.VMEM((SLOTS, TILE // part, own, part), jnp.bfloat16),
                pltpu.VMEM((n, 3, own, part), jnp.bfloat16),
                pltpu.VMEM((PER, n, HEAD, own), jnp.bfloat16),
                pltpu.VMEM((2, n, own, part), jnp.bfloat16),
                pltpu.VMEM((2, own, TILE), jnp.bfloat16),
                pltpu.SemaphoreType.DMA((1,)),
                pltpu.SemaphoreType.DMA((2,)),
                pltpu.SemaphoreType.DMA((SLOTS, TILE // part)),
                pltpu.SemaphoreType.DMA((rounds, n)),
                pltpu.SemaphoreType.DMA((n,)),
                pltpu.SemaphoreType.DMA((2, n)),
                pltpu.SemaphoreType.DMA((rounds, n)),
                pltpu.SemaphoreType.DMA((2,)),
                pltpu.SemaphoreType.DMA((2,)),
            ],
            compiler_params=pltpu.CompilerParams(collective_id=0, has_side_effects=True, vmem_limit_bytes=67043328),
        )(x, gain[None], cos, sin, wq, wk, wv, wo)
        return y

    tokens, whole = P(("dp", "sp"), None), P(None, None)
    return jax.shard_map(
        step,
        mesh=mesh,
        in_specs=(tokens, P(None), whole, whole, whole, whole),
        out_specs=tokens,
        check_vma=False,
    )
```

```python
import functools

import jax
import jax.numpy as jnp
from jax import lax
from jax.experimental import pallas as pl
from jax.experimental.pallas import tpu as pltpu
from jax.sharding import PartitionSpec as P

HEAD = 128
THETA = 10000
LOG2E = 1.4426950408889634
MESH = pl.DeviceIdType.MESH
PER = 2
TILE = 512
SLOTS = 12
HIDDEN = -1e30


def _dot(a, b, ca, cb):
    return lax.dot_general(a, b, (((ca,), (cb,)), ((), ())), preferred_element_type=jnp.float32)


def _kernel(n, x_hbm, gain_ref, cos_ref, sin_ref, wq, wk, wv, wo, y_hbm, qkv_hbm, o_hbm, own_hbm, lse_hbm,
            a, w, acc, raw, out, qkv, vt, o, xt, mine, held, lse_in, lse_out, kept, kept_lse,
            asem, wsem, csend, crecv, lsem, dsend, drecv, xsem, ysem, esem, fsem, gsem, hsem, osem, lsend, lrecv):
    me = lax.axis_index("sp")
    dp = lax.axis_index("dp")
    own, width = a.shape
    part = PER * HEAD
    span = n * part
    rounds = width // span
    ntile = width // TILE
    per_round = 3 * (span // TILE)
    homes = TILE // part
    tiles = rounds * per_round
    end = jnp.logical_or(me == 0, me == n - 1)
    groups = [(0, rounds - 2), (rounds - 2, rounds - 1), (rounds - 1, rounds)]

    barrier = pltpu.get_barrier_semaphore()
    for s in range(1, n):
        pl.semaphore_signal(barrier, inc=1, device_id=(dp, lax.rem(me + s, n)), device_id_type=MESH)

    def w_copy(ref, i, slot):
        return pltpu.make_async_copy(ref.at[:, pl.ds(pl.multiple_of(i * TILE, TILE), TILE)], w.at[slot], wsem.at[slot])

    def w_start(i):
        for t, ref in enumerate((wk, wv, wq)):
            @pl.when(lax.rem(i, 3) == t)
            def _():
                w_copy(ref, lax.div(i, 3), lax.rem(i, 2)).start()

    def wo_copy(g, j):
        lo, hi = groups[g][0] * span, groups[g][1] * span
        slot = lax.rem(j, 2)
        return pltpu.make_async_copy(wo.at[pl.ds(lo, hi - lo), pl.ds(pl.multiple_of(j * TILE, TILE), TILE)],
                                     w.at[slot, pl.ds(0, hi - lo)], wsem.at[slot])

    w_start(jnp.int32(0))
    w_start(jnp.int32(1))
    strip = 16
    load = pltpu.make_async_copy(x_hbm, a, asem.at[0])
    load.start()
    raw[1] = jnp.zeros_like(raw[1])
    lse_out[...] = jnp.zeros_like(lse_out)
    load.wait()

    def norm(i, _):
        rows = pl.ds(pl.multiple_of(i * strip, strip), strip)
        sums = jnp.zeros((strip, 128), jnp.float32)
        for c in range(0, width, 512):
            v = a[rows, c : c + 512].astype(jnp.float32)
            v = v * v
            sums = sums + ((v[:, :128] + v[:, 128:256]) + (v[:, 256:384] + v[:, 384:]))
        scale = lax.rsqrt(jnp.sum(sums, -1, keepdims=True) / width + 1e-6)
        for c in range(0, width, 512):
            v = a[rows, c : c + 512].astype(jnp.float32)
            a[rows, c : c + 512] = (v * scale * gain_ref[:, c : c + 512].astype(jnp.float32)).astype(jnp.bfloat16)
        return 0

    lax.fori_loop(0, own // strip, norm, 0)
    pl.semaphore_wait(barrier, n - 1)

    def tile_of(i):
        return lax.div(i, per_round), lax.rem(i, 3), lax.rem(lax.div(i, 3), span // TILE) * homes

    def c_copy(i, e):
        r, t, home = tile_of(i)
        slot = lax.rem(i, SLOTS)
        return pltpu.make_async_remote_copy(out.at[slot, e], qkv_hbm.at[r, me, t], csend.at[slot, e], crecv.at[r, me],
                                            device_id=(dp, home + e), device_id_type=MESH)

    def c_own(i, e):
        r, t, home = tile_of(i)
        return pltpu.make_async_copy(out.at[lax.rem(i, SLOTS), e], qkv_hbm.at[r, me, t], crecv.at[r, me])

    def needed(i):
        query = lax.rem(i, 3) == 2
        return jnp.logical_not(jnp.logical_or(jnp.logical_and(query, me == 0), jnp.logical_and(jnp.logical_not(query), me == n - 1)))

    def e_copy(i, e):
        r, t, home = tile_of(i)
        slot = lax.rem(i, SLOTS)
        return pltpu.make_async_copy(out.at[slot, e], own_hbm.at[r, home + e, t], esem.at[slot, e])

    def c_send(i):
        for e in range(homes):
            there = tile_of(i)[2] + e

            @pl.when(jnp.logical_and(there != me, needed(i)))
            def _():
                c_copy(i, e).start()

            @pl.when(there == me)
            def _():
                c_own(i, e).start()

            @pl.when(end)
            def _():
                e_copy(i, e).start()

    def c_sent(i):
        for e in range(homes):
            @pl.when(jnp.logical_and(tile_of(i)[2] + e != me, needed(i)))
            def _():
                c_copy(i, e).wait_send()

    def e_sent(i):
        @pl.when(end)
        def _():
            for e in range(homes):
                e_copy(i, e).wait()

    def turn(i, par):
        t = lax.rem(i, 3)
        kind = lax.select(t == 1, 1, 0)
        slot = lax.rem(i, SLOTS)
        for c in range(TILE // HEAD):
            v = raw[par, :, c * HEAD : (c + 1) * HEAD].astype(jnp.float32)
            v = v * cos_ref[kind] + pltpu.roll(v, HEAD // 2, 1) * sin_ref[kind]
            e, at = c // PER, c % PER * HEAD
            out[slot, e, :, at : at + HEAD] = v.astype(jnp.bfloat16)

    def project(i, par):
        w_copy(wq, 0, par).wait()

        @pl.when(i > SLOTS)
        def _():
            c_sent(i - 1 - SLOTS)

        before = lax.rem(i + tiles * SLOTS - 1, tiles * SLOTS)
        raw[par] = jnp.dot(a[...], w[par], preferred_element_type=jnp.float32).astype(jnp.bfloat16)
        turn(before, 1 - par)

        @pl.when(i > 0)
        def _():
            c_send(i - 1)

        @pl.when(i > 2)
        def _():
            e_sent(i - 3)

        @pl.when(i + 2 < tiles)
        def _():
            w_start(i + 2)

        @pl.when(i + 2 >= tiles)
        def _():
            wo_copy(0, i + 2 - tiles).start()

    e2 = HEAD**-0.5 * LOG2E

    def columns(r, s):
        return o_hbm.at[:, pl.ds(pl.multiple_of(r * span + s * part, part), part)]

    def d_copy(r, b):
        slot = lax.rem(r, 2)
        return pltpu.make_async_remote_copy(o.at[slot, b - 1], columns(r, me), dsend.at[slot, b], drecv.at[r, me],
                                            device_id=(dp, b), device_id_type=MESH)

    def d_own(r, b):
        return pltpu.make_async_copy(o.at[lax.rem(r, 2), b - 1], columns(r, me), drecv.at[r, me])

    def l_copy(r):
        slot = lax.rem(r, 2)
        return pltpu.make_async_remote_copy(lse_out.at[slot], lse_hbm.at[r, me], lsend.at[slot], lrecv.at[r, me],
                                            device_id=(dp, n - 1), device_id_type=MESH)

    def d_start(r):
        for b in range(1, n):
            @pl.when(b != me)
            def _():
                d_copy(r, b).start()
        for b in range(1, n - 1):
            @pl.when(b == me)
            def _():
                d_own(r, b).start()

        @pl.when(me != n - 1)
        def _():
            l_copy(r).start()

    def d_sent(r):
        for b in range(1, n):
            @pl.when(b != me)
            def _():
                d_copy(r, b).wait_send()

        @pl.when(me != n - 1)
        def _():
            l_copy(r).wait_send()

    def own_sent(r):
        @pl.when(jnp.logical_not(end))
        def _():
            d_own(r, 1).wait()

    def fetch(r):
        for s in range(n):
            lo, hi = (0, 2) if s == 0 else (2, 3) if s == n - 1 else (0, 3)

            def arrived(lo, hi, s=s):
                at = qkv_hbm.at[r, s, pl.ds(lo, hi - lo)]
                pltpu.make_async_copy(at, at, crecv.at[r, s]).wait()
                pltpu.make_async_copy(at, qkv.at[s, pl.ds(lo, hi - lo)], lsem.at[s]).start()

            if hi - lo == 3:
                arrived(0, 3)
            else:
                pl.when(s == me)(functools.partial(arrived, 0, 3))
                pl.when(s != me)(functools.partial(arrived, lo, hi))

    def fetched():
        for s in range(n):
            lo, hi = (0, 2) if s == 0 else (2, 3) if s == n - 1 else (0, 3)

            def arrived(lo, hi, s=s):
                pltpu.make_async_copy(qkv_hbm.at[0, s, pl.ds(lo, hi - lo)], qkv.at[s, pl.ds(lo, hi - lo)], lsem.at[s]).wait()

            if hi - lo == 3:
                arrived(0, 3)
            else:
                pl.when(s == me)(functools.partial(arrived, 0, 3))
                pl.when(s != me)(functools.partial(arrived, lo, hi))

    def seen():
        return lax.broadcasted_iota(jnp.int32, (own, own), 0) <= lax.broadcasted_iota(jnp.int32, (own, own), 1)

    def attend(r):
        @pl.when(r >= 1)
        def _():
            own_sent(r - 1)

        @pl.when(r >= 2)
        def _():
            d_sent(r - 2)

        fetched()
        slot = lax.rem(r, 2)
        ok = seen()
        for h in range(PER):
            for j in range(n - 1):
                vt[h, j] = qkv[j, 1, :, h * HEAD : (h + 1) * HEAD].T
        pieces = [(h, i) for i in range(1, n) for h in range(PER)]

        def scores(h, i):
            q = qkv[i, 2, :, h * HEAD : (h + 1) * HEAD]
            s = [_dot(qkv[j, 0, :, h * HEAD : (h + 1) * HEAD], q, 1, 1) for j in range(min(i + 1, n - 1))]
            if i < n - 1:
                s[i] = jnp.where(ok, s[i], HIDDEN)
            return s

        ahead = scores(*pieces[0])
        for k, (h, i) in enumerate(pieces):
            s = ahead
            if k + 1 < len(pieces):
                ahead = scores(*pieces[k + 1])
            top = functools.reduce(jnp.maximum, [t.max(axis=0, keepdims=True) for t in s]) * e2
            total, mix = 0.0, 0.0
            for j, t in enumerate(s):
                p = jnp.exp2(t * e2 - top)
                total = total + p.sum(axis=0, keepdims=True)
                mix = mix + _dot(vt[h, j], p.astype(jnp.bfloat16), 1, 0)
            mix = mix * (1 / total)
            if i == n - 1:
                kept[slot, h] = mix
                log = top + jnp.log2(total)
                lse_out[slot, h : h + 1, :] = log
                kept_lse[slot, h : h + 1, :] = log
            o[slot, i - 1, :, h * HEAD : (h + 1) * HEAD] = mix.T.astype(jnp.bfloat16)
        d_start(r)

    def h_copy(r, s):
        return pltpu.make_async_copy(held.at[s], columns(r, s), osem.at[s])

    def own_fetch(r):
        for s in range(n):
            pltpu.make_async_copy(own_hbm.at[r, s], mine.at[s], fsem.at[s]).start()

    def own_done(r):
        for s in range(n):
            h_copy(r, s).wait()

    def own_attend(r):
        @pl.when(me == n - 1)
        def _():
            for s in range(n - 1):
                pltpu.make_async_copy(columns(r, s), columns(r, s), drecv.at[r, s]).wait()
                pltpu.make_async_copy(columns(r, s), held.at[s], gsem.at[s]).start()
                pltpu.make_async_copy(lse_hbm.at[r, s], lse_hbm.at[r, s], lrecv.at[r, s]).wait()
                pltpu.make_async_copy(lse_hbm.at[r, s], lse_in.at[s], hsem.at[s]).start()
            for s in range(n - 1):
                pltpu.make_async_copy(columns(r, s), held.at[s], gsem.at[s]).wait()
                pltpu.make_async_copy(lse_hbm.at[r, s], lse_in.at[s], hsem.at[s]).wait()

        for s in range(n):
            pltpu.make_async_copy(own_hbm.at[r, s], mine.at[s], fsem.at[s]).wait()
        slot = lax.rem(r, 2)
        ok = seen()
        pieces = [(s, h) for s in range(n) for h in range(PER)]

        def scores(s, h):
            at = slice(h * HEAD, (h + 1) * HEAD)
            return jnp.where(ok, _dot(mine[s, 0, :, at], mine[s, 2, :, at], 1, 1), HIDDEN)

        ahead = scores(*pieces[0])
        for k, (s, h) in enumerate(pieces):
            t = ahead
            if k + 1 < len(pieces):
                ahead = scores(*pieces[k + 1])
            at = slice(h * HEAD, (h + 1) * HEAD)
            if s == n - 1:
                before, log = kept[slot, h], kept_lse[slot, h : h + 1, :]
            else:
                before, log = held[s, :, at].astype(jnp.float32).T, lse_in[s, h : h + 1, :]
            before, log = jnp.where(me == 0, 0.0, before), jnp.where(me == 0, HIDDEN, log)
            top = jnp.maximum(t.max(axis=0, keepdims=True) * e2, log)
            p = jnp.exp2(t * e2 - top)
            keep = jnp.exp2(log - top)
            total = p.sum(axis=0, keepdims=True) + keep
            mix = before * keep + _dot(mine[s, 1, :, at].T, p.astype(jnp.bfloat16), 1, 0)
            held[s, :, at] = (mix * (1 / total)).T.astype(jnp.bfloat16)
        for s in range(n):
            h_copy(r, s).start()

    def x_copy(j):
        slot = lax.rem(j, 2)
        return pltpu.make_async_copy(x_hbm.at[:, pl.ds(pl.multiple_of(j * TILE, TILE), TILE)], xt.at[slot], xsem.at[slot])

    def y_copy(j):
        slot = lax.rem(j, 2)
        return pltpu.make_async_copy(raw.at[slot], y_hbm.at[:, pl.ds(pl.multiple_of(j * TILE, TILE), TILE)], ysem.at[slot])

    def combine(g):
        lo, hi = groups[g][0] * span, groups[g][1] * span
        @pl.when(jnp.logical_not(end))
        def _():
            for r in range(*groups[g]):
                for s in range(n):
                    @pl.when(s != me)
                    def _():
                        pltpu.make_async_copy(columns(r, s), columns(r, s), drecv.at[r, s]).wait()
        load = pltpu.make_async_copy(o_hbm.at[:, pl.ds(lo, hi - lo)], a.at[:, pl.ds(lo, hi - lo)], asem.at[0])
        load.start()
        last = g == len(groups) - 1
        if last:
            x_copy(0).start()
            x_copy(1).start()
        load.wait()

        def body(j, _):
            slot = lax.rem(j, 2)
            wo_copy(g, j).wait()
            if last:
                x_copy(j).wait()

                @pl.when(j >= 2)
                def _():
                    y_copy(j - 2).wait()
            got = jnp.dot(a[:, lo:hi], w[slot, : hi - lo], preferred_element_type=jnp.float32)
            if g:
                got = got + acc[j]
            if last:
                raw[slot] = (xt[slot].astype(jnp.float32) + got).astype(jnp.bfloat16)
                y_copy(j).start()
            else:
                acc[j] = got

            @pl.when(j + 2 < ntile)
            def _():
                wo_copy(g, j + 2).start()
                if last:
                    x_copy(j + 2).start()
            if not last:
                @pl.when(j + 2 >= ntile)
                def _():
                    wo_copy(g + 1, j + 2 - ntile).start()
            return 0

        lax.fori_loop(0, ntile, body, 0)
        if last:
            y_copy(ntile - 2).wait()
            y_copy(ntile - 1).wait()

    def step(r, _):
        @pl.when(r < rounds)
        def _():
            def one(k, _):
                @pl.when(jnp.logical_and(k == per_round // 2 - 1, r > 0))
                def _():
                    fetch(r - 1)

                project(r * per_round + 2 * k, 0)
                project(r * per_round + 2 * k + 1, 1)
                return 0

            lax.fori_loop(0, per_round // 2, one, 0)

        @pl.when(r == rounds - 1)
        def _():
            c_sent(jnp.int32(tiles - 1 - SLOTS))
            turn(jnp.int32(tiles - 1), (tiles - 1) % 2)
            c_send(jnp.int32(tiles - 1))
            for i in range(tiles - 3, tiles):
                e_sent(jnp.int32(i))

        @pl.when(jnp.logical_and(r > 2, end))
        def _():
            own_done(r - 3)

        @pl.when(r == rounds)
        def _():
            combine(0)
            fetch(r - 1)

        @pl.when(jnp.logical_and(r > 1, end))
        def _():
            own_fetch(r - 2)

        @pl.when(r > 0)
        def _():
            attend(r - 1)

        @pl.when(jnp.logical_and(r > 1, end))
        def _():
            own_attend(r - 2)

        return 0

    lax.fori_loop(0, rounds + 1, step, 0)
    own_sent(rounds - 1)

    @pl.when(end)
    def _():
        own_done(rounds - 2)
        own_fetch(rounds - 1)

    combine(1)

    @pl.when(end)
    def _():
        own_attend(rounds - 1)
        own_done(rounds - 1)

    combine(2)
    for i in range(tiles - SLOTS, tiles):
        c_sent(jnp.int32(i))
    d_sent(rounds - 2)
    d_sent(rounds - 1)


def solution(mesh):
    n = mesh.shape["sp"]

    def step(x, gain, wq, wk, wv, wo):
        own, width = x.shape
        part = PER * HEAD
        rounds = width // (n * part)
        place = lax.axis_index("sp") * own + jnp.arange(own)
        half = HEAD // 2
        angle = place.astype(jnp.float32)[:, None] * THETA ** (-jnp.arange(half, dtype=jnp.float32) / half)
        cos, sin = jnp.cos(angle), jnp.sin(angle)
        one = jnp.ones((own, HEAD), jnp.float32)
        cos = jnp.stack([jnp.concatenate([cos, cos], -1), one])
        sin = jnp.stack([jnp.concatenate([-sin, sin], -1), 0 * one])
        anywhere, vmem = pl.BlockSpec(memory_space=pl.ANY), pl.BlockSpec(memory_space=pltpu.VMEM)
        y, *_ = pl.pallas_call(
            functools.partial(_kernel, n),
            out_shape=[jax.ShapeDtypeStruct((own, width), jnp.bfloat16),
                       jax.ShapeDtypeStruct((rounds, n, 3, own, part), jnp.bfloat16),
                       jax.ShapeDtypeStruct((own, width), jnp.bfloat16),
                       jax.ShapeDtypeStruct((rounds, n, 3, own, part), jnp.bfloat16),
                       jax.ShapeDtypeStruct((rounds, n, 8, own), jnp.float32)],
            in_specs=[anywhere, vmem, vmem, vmem] + [anywhere] * 4,
            out_specs=[anywhere] * 5,
            scratch_shapes=[
                pltpu.VMEM((own, width), jnp.bfloat16),
                pltpu.VMEM((2, width, TILE), jnp.bfloat16),
                pltpu.VMEM((width // TILE, own, TILE), jnp.float32),
                pltpu.VMEM((2, own, TILE), jnp.bfloat16),
                pltpu.VMEM((SLOTS, TILE // part, own, part), jnp.bfloat16),
                pltpu.VMEM((n, 3, own, part), jnp.bfloat16),
                pltpu.VMEM((PER, n, HEAD, own), jnp.bfloat16),
                pltpu.VMEM((2, n - 1, own, part), jnp.bfloat16),
                pltpu.VMEM((2, own, TILE), jnp.bfloat16),
                pltpu.VMEM((n, 3, own, part), jnp.bfloat16),
                pltpu.VMEM((n, own, part), jnp.bfloat16),
                pltpu.VMEM((n, 8, own), jnp.float32),
                pltpu.VMEM((2, 8, own), jnp.float32),
                pltpu.VMEM((2, PER, HEAD, own), jnp.float32),
                pltpu.VMEM((2, 8, own), jnp.float32),
                pltpu.SemaphoreType.DMA((1,)),
                pltpu.SemaphoreType.DMA((2,)),
                pltpu.SemaphoreType.DMA((SLOTS, TILE // part)),
                pltpu.SemaphoreType.DMA((rounds, n)),
                pltpu.SemaphoreType.DMA((n,)),
                pltpu.SemaphoreType.DMA((2, n)),
                pltpu.SemaphoreType.DMA((rounds, n)),
                pltpu.SemaphoreType.DMA((2,)),
                pltpu.SemaphoreType.DMA((2,)),
                pltpu.SemaphoreType.DMA((SLOTS, TILE // part)),
                pltpu.SemaphoreType.DMA((n,)),
                pltpu.SemaphoreType.DMA((n,)),
                pltpu.SemaphoreType.DMA((n,)),
                pltpu.SemaphoreType.DMA((n,)),
                pltpu.SemaphoreType.DMA((2,)),
                pltpu.SemaphoreType.DMA((rounds, n)),
            ],
            compiler_params=pltpu.CompilerParams(collective_id=0, has_side_effects=True, vmem_limit_bytes=67043328),
        )(x, gain[None], cos, sin, wq, wk, wv, wo)
        return y

    tokens, whole = P(("dp", "sp"), None), P(None, None)
    return jax.shard_map(
        step,
        mesh=mesh,
        in_specs=(tokens, P(None), whole, whole, whole, whole),
        out_specs=tokens,
        check_vma=False,
    )
```

```python
import functools

import jax
import jax.numpy as jnp
from jax import lax
from jax.experimental import pallas as pl
from jax.experimental.pallas import tpu as pltpu
from jax.sharding import PartitionSpec as P

HEAD = 128
THETA = 10000
LOG2E = 1.4426950408889634
MESH = pl.DeviceIdType.MESH
PER = 2
TILE = 512
SLOTS = 12
HIDDEN = -1e30


def _dot(a, b, ca, cb):
    return lax.dot_general(a, b, (((ca,), (cb,)), ((), ())), preferred_element_type=jnp.float32)


def _kernel(n, x_hbm, gain_ref, cos_ref, sin_ref, wq, wk, wv, wo, y_hbm, qkv_hbm, o_hbm, own_hbm, lse_hbm,
            a, w, acc, raw, out, qkv, vt, o, xt, mine, held, lse_in, lse_out, kept, kept_lse,
            asem, wsem, csend, crecv, lsem, dsend, drecv, xsem, ysem, esem, fsem, gsem, hsem, osem, lsend, lrecv):
    me = lax.axis_index("sp")
    dp = lax.axis_index("dp")
    own, width = a.shape
    part = PER * HEAD
    span = n * part
    rounds = width // span
    ntile = width // TILE
    per_round = 3 * (span // TILE)
    homes = TILE // part
    tiles = rounds * per_round
    end = jnp.logical_or(me == 0, me == n - 1)
    groups = [(0, rounds - 2), (rounds - 2, rounds - 1), (rounds - 1, rounds)]

    barrier = pltpu.get_barrier_semaphore()
    for s in range(1, n):
        pl.semaphore_signal(barrier, inc=1, device_id=(dp, lax.rem(me + s, n)), device_id_type=MESH)

    def w_copy(ref, i, slot):
        return pltpu.make_async_copy(ref.at[:, pl.ds(pl.multiple_of(i * TILE, TILE), TILE)], w.at[slot], wsem.at[slot])

    def w_start(i):
        for t, ref in enumerate((wk, wv, wq)):
            @pl.when(lax.rem(i, 3) == t)
            def _():
                w_copy(ref, lax.div(i, 3), lax.rem(i, 2)).start()

    def wo_copy(g, j):
        lo, hi = groups[g][0] * span, groups[g][1] * span
        slot = lax.rem(j, 2)
        return pltpu.make_async_copy(wo.at[pl.ds(lo, hi - lo), pl.ds(pl.multiple_of(j * TILE, TILE), TILE)],
                                     w.at[slot, pl.ds(0, hi - lo)], wsem.at[slot])

    w_start(jnp.int32(0))
    w_start(jnp.int32(1))
    strip = 16
    load = pltpu.make_async_copy(x_hbm, a, asem.at[0])
    load.start()
    raw[1] = jnp.zeros_like(raw[1])
    lse_out[...] = jnp.zeros_like(lse_out)
    load.wait()

    def norm(i, _):
        rows = pl.ds(pl.multiple_of(i * strip, strip), strip)
        sums = jnp.zeros((strip, 128), jnp.float32)
        for c in range(0, width, 512):
            v = a[rows, c : c + 512].astype(jnp.float32)
            v = v * v
            sums = sums + ((v[:, :128] + v[:, 128:256]) + (v[:, 256:384] + v[:, 384:]))
        scale = lax.rsqrt(jnp.sum(sums, -1, keepdims=True) / width + 1e-6)
        for c in range(0, width, 512):
            v = a[rows, c : c + 512].astype(jnp.float32)
            a[rows, c : c + 512] = (v * scale * gain_ref[:, c : c + 512].astype(jnp.float32)).astype(jnp.bfloat16)
        return 0

    lax.fori_loop(0, own // strip, norm, 0)
    pl.semaphore_wait(barrier, n - 1)

    def tile_of(i):
        return lax.div(i, per_round), lax.rem(i, 3), lax.rem(lax.div(i, 3), span // TILE) * homes

    def group_of(i):
        return lax.rem(lax.div(i, 3), SLOTS // 3)

    def c_copy(i, e, lo, hi):
        r, _, home = tile_of(i)
        g, parts = group_of(i), pl.ds(lo, hi - lo)
        return pltpu.make_async_remote_copy(out.at[g, e, parts], qkv_hbm.at[r, me, parts], csend.at[g, e], crecv.at[r, me],
                                            device_id=(dp, home + e), device_id_type=MESH)

    def c_own(i, e):
        return pltpu.make_async_copy(out.at[group_of(i), e], qkv_hbm.at[tile_of(i)[0], me], crecv.at[tile_of(i)[0], me])

    def e_copy(i, e):
        r, _, home = tile_of(i)
        return pltpu.make_async_copy(out.at[group_of(i), e], own_hbm.at[r, home + e], esem.at[group_of(i), e])

    sends = ((me == 0, 0, 2), (me == n - 1, 2, 3), (jnp.logical_not(end), 0, 3))

    def c_send(i):
        for e in range(homes):
            there = tile_of(i)[2] + e
            for who, lo, hi in sends:
                @pl.when(jnp.logical_and(there != me, who))
                def _():
                    c_copy(i, e, lo, hi).start()

            @pl.when(there == me)
            def _():
                c_own(i, e).start()

            @pl.when(end)
            def _():
                e_copy(i, e).start()

    def c_sent(i):
        for e in range(homes):
            for who, lo, hi in sends:
                @pl.when(jnp.logical_and(tile_of(i)[2] + e != me, who))
                def _():
                    c_copy(i, e, lo, hi).wait_send()

    def e_sent(i):
        @pl.when(end)
        def _():
            for e in range(homes):
                e_copy(i, e).wait()

    def turn(i, par):
        t = lax.rem(i, 3)
        kind = lax.select(t == 1, 1, 0)
        g = group_of(i)
        for c in range(TILE // HEAD):
            v = raw[par, :, c * HEAD : (c + 1) * HEAD].astype(jnp.float32)
            v = v * cos_ref[kind] + pltpu.roll(v, HEAD // 2, 1) * sin_ref[kind]
            e, at = c // PER, c % PER * HEAD
            out[g, e, t, :, at : at + HEAD] = v.astype(jnp.bfloat16)

    def project(i, par):
        w_copy(wq, 0, par).wait()

        @pl.when(jnp.logical_and(i > SLOTS, lax.rem(i, 3) == 1))
        def _():
            c_sent(i - 1 - SLOTS)

        before = lax.rem(i + tiles * SLOTS - 1, tiles * SLOTS)
        raw[par] = jnp.dot(a[...], w[par], preferred_element_type=jnp.float32).astype(jnp.bfloat16)
        turn(before, 1 - par)

        @pl.when(jnp.logical_and(i > 0, lax.rem(i, 3) == 0))
        def _():
            c_send(i - 1)

        @pl.when(jnp.logical_and(i > 2, lax.rem(i, 3) == 2))
        def _():
            e_sent(i - 3)

        @pl.when(i + 2 < tiles)
        def _():
            w_start(i + 2)

        @pl.when(i + 2 >= tiles)
        def _():
            wo_copy(0, i + 2 - tiles).start()

    e2 = HEAD**-0.5 * LOG2E

    def columns(r, s):
        return o_hbm.at[:, pl.ds(pl.multiple_of(r * span + s * part, part), part)]

    def d_copy(r, b):
        slot = lax.rem(r, 2)
        return pltpu.make_async_remote_copy(o.at[slot, b - 1], columns(r, me), dsend.at[slot, b], drecv.at[r, me],
                                            device_id=(dp, b), device_id_type=MESH)

    def d_own(r, b):
        return pltpu.make_async_copy(o.at[lax.rem(r, 2), b - 1], columns(r, me), drecv.at[r, me])

    def l_copy(r):
        slot = lax.rem(r, 2)
        return pltpu.make_async_remote_copy(lse_out.at[slot], lse_hbm.at[r, me], lsend.at[slot], lrecv.at[r, me],
                                            device_id=(dp, n - 1), device_id_type=MESH)

    def d_start(r):
        for b in range(1, n):
            @pl.when(b != me)
            def _():
                d_copy(r, b).start()
        for b in range(1, n - 1):
            @pl.when(b == me)
            def _():
                d_own(r, b).start()

        @pl.when(me != n - 1)
        def _():
            l_copy(r).start()

    def d_sent(r):
        for b in range(1, n):
            @pl.when(b != me)
            def _():
                d_copy(r, b).wait_send()

        @pl.when(me != n - 1)
        def _():
            l_copy(r).wait_send()

    def own_sent(r):
        @pl.when(jnp.logical_not(end))
        def _():
            d_own(r, 1).wait()

    def fetch(r):
        for s in range(n):
            lo, hi = (0, 2) if s == 0 else (2, 3) if s == n - 1 else (0, 3)

            def arrived(lo, hi, s=s):
                at = qkv_hbm.at[r, s, pl.ds(lo, hi - lo)]
                pltpu.make_async_copy(at, at, crecv.at[r, s]).wait()
                pltpu.make_async_copy(at, qkv.at[s, pl.ds(lo, hi - lo)], lsem.at[s]).start()

            if hi - lo == 3:
                arrived(0, 3)
            else:
                pl.when(s == me)(functools.partial(arrived, 0, 3))
                pl.when(s != me)(functools.partial(arrived, lo, hi))

    def fetched():
        for s in range(n):
            lo, hi = (0, 2) if s == 0 else (2, 3) if s == n - 1 else (0, 3)

            def arrived(lo, hi, s=s):
                pltpu.make_async_copy(qkv_hbm.at[0, s, pl.ds(lo, hi - lo)], qkv.at[s, pl.ds(lo, hi - lo)], lsem.at[s]).wait()

            if hi - lo == 3:
                arrived(0, 3)
            else:
                pl.when(s == me)(functools.partial(arrived, 0, 3))
                pl.when(s != me)(functools.partial(arrived, lo, hi))

    def seen():
        return lax.broadcasted_iota(jnp.int32, (own, own), 0) <= lax.broadcasted_iota(jnp.int32, (own, own), 1)

    def attend(r):
        @pl.when(r >= 1)
        def _():
            own_sent(r - 1)

        @pl.when(r >= 2)
        def _():
            d_sent(r - 2)

        fetched()
        slot = lax.rem(r, 2)
        ok = seen()
        for h in range(PER):
            for j in range(n - 1):
                vt[h, j] = qkv[j, 1, :, h * HEAD : (h + 1) * HEAD].T
        pieces = [(h, i) for i in range(1, n) for h in range(PER)]

        def scores(h, i):
            q = qkv[i, 2, :, h * HEAD : (h + 1) * HEAD]
            s = [_dot(qkv[j, 0, :, h * HEAD : (h + 1) * HEAD], q, 1, 1) for j in range(min(i + 1, n - 1))]
            if i < n - 1:
                s[i] = jnp.where(ok, s[i], HIDDEN)
            return s

        ahead = scores(*pieces[0])
        for k, (h, i) in enumerate(pieces):
            s = ahead
            if k + 1 < len(pieces):
                ahead = scores(*pieces[k + 1])
            top = functools.reduce(jnp.maximum, [t.max(axis=0, keepdims=True) for t in s]) * e2
            total, mix = 0.0, 0.0
            for j, t in enumerate(s):
                p = jnp.exp2(t * e2 - top)
                total = total + p.sum(axis=0, keepdims=True)
                mix = mix + _dot(vt[h, j], p.astype(jnp.bfloat16), 1, 0)
            mix = mix * (1 / total)
            if i == n - 1:
                kept[slot, h] = mix
                log = top + jnp.log2(total)
                lse_out[slot, h : h + 1, :] = log
                kept_lse[slot, h : h + 1, :] = log
            o[slot, i - 1, :, h * HEAD : (h + 1) * HEAD] = mix.T.astype(jnp.bfloat16)
        d_start(r)

    def h_copy(r, s):
        return pltpu.make_async_copy(held.at[s], columns(r, s), osem.at[s])

    def own_fetch(r):
        for s in range(n):
            pltpu.make_async_copy(own_hbm.at[r, s], mine.at[s], fsem.at[s]).start()

    def own_done(r):
        for s in range(n):
            h_copy(r, s).wait()

    def own_attend(r):
        @pl.when(me == n - 1)
        def _():
            for s in range(n - 1):
                pltpu.make_async_copy(columns(r, s), columns(r, s), drecv.at[r, s]).wait()
                pltpu.make_async_copy(columns(r, s), held.at[s], gsem.at[s]).start()
                pltpu.make_async_copy(lse_hbm.at[r, s], lse_hbm.at[r, s], lrecv.at[r, s]).wait()
                pltpu.make_async_copy(lse_hbm.at[r, s], lse_in.at[s], hsem.at[s]).start()
            for s in range(n - 1):
                pltpu.make_async_copy(columns(r, s), held.at[s], gsem.at[s]).wait()
                pltpu.make_async_copy(lse_hbm.at[r, s], lse_in.at[s], hsem.at[s]).wait()

        for s in range(n):
            pltpu.make_async_copy(own_hbm.at[r, s], mine.at[s], fsem.at[s]).wait()
        slot = lax.rem(r, 2)
        ok = seen()
        pieces = [(s, h) for s in range(n) for h in range(PER)]

        def scores(s, h):
            at = slice(h * HEAD, (h + 1) * HEAD)
            return jnp.where(ok, _dot(mine[s, 0, :, at], mine[s, 2, :, at], 1, 1), HIDDEN)

        ahead = scores(*pieces[0])
        for k, (s, h) in enumerate(pieces):
            t = ahead
            if k + 1 < len(pieces):
                ahead = scores(*pieces[k + 1])
            at = slice(h * HEAD, (h + 1) * HEAD)
            if s == n - 1:
                before, log = kept[slot, h], kept_lse[slot, h : h + 1, :]
            else:
                before, log = held[s, :, at].astype(jnp.float32).T, lse_in[s, h : h + 1, :]
            before, log = jnp.where(me == 0, 0.0, before), jnp.where(me == 0, HIDDEN, log)
            top = jnp.maximum(t.max(axis=0, keepdims=True) * e2, log)
            p = jnp.exp2(t * e2 - top)
            keep = jnp.exp2(log - top)
            total = p.sum(axis=0, keepdims=True) + keep
            mix = before * keep + _dot(mine[s, 1, :, at].T, p.astype(jnp.bfloat16), 1, 0)
            held[s, :, at] = (mix * (1 / total)).T.astype(jnp.bfloat16)
        for s in range(n):
            h_copy(r, s).start()

    def x_copy(j):
        slot = lax.rem(j, 2)
        return pltpu.make_async_copy(x_hbm.at[:, pl.ds(pl.multiple_of(j * TILE, TILE), TILE)], xt.at[slot], xsem.at[slot])

    def y_copy(j):
        slot = lax.rem(j, 2)
        return pltpu.make_async_copy(raw.at[slot], y_hbm.at[:, pl.ds(pl.multiple_of(j * TILE, TILE), TILE)], ysem.at[slot])

    def combine(g):
        lo, hi = groups[g][0] * span, groups[g][1] * span
        @pl.when(jnp.logical_not(end))
        def _():
            for r in range(*groups[g]):
                for s in range(n):
                    @pl.when(s != me)
                    def _():
                        pltpu.make_async_copy(columns(r, s), columns(r, s), drecv.at[r, s]).wait()
        load = pltpu.make_async_copy(o_hbm.at[:, pl.ds(lo, hi - lo)], a.at[:, pl.ds(lo, hi - lo)], asem.at[0])
        load.start()
        last = g == len(groups) - 1
        if last:
            x_copy(0).start()
            x_copy(1).start()
        load.wait()

        def body(j, _):
            slot = lax.rem(j, 2)
            wo_copy(g, j).wait()
            if last:
                x_copy(j).wait()

                @pl.when(j >= 2)
                def _():
                    y_copy(j - 2).wait()
            got = jnp.dot(a[:, lo:hi], w[slot, : hi - lo], preferred_element_type=jnp.float32)
            if g:
                got = got + acc[j]
            if last:
                raw[slot] = (xt[slot].astype(jnp.float32) + got).astype(jnp.bfloat16)
                y_copy(j).start()
            else:
                acc[j] = got

            @pl.when(j + 2 < ntile)
            def _():
                wo_copy(g, j + 2).start()
                if last:
                    x_copy(j + 2).start()
            if not last:
                @pl.when(j + 2 >= ntile)
                def _():
                    wo_copy(g + 1, j + 2 - ntile).start()
            return 0

        lax.fori_loop(0, ntile, body, 0)
        if last:
            y_copy(ntile - 2).wait()
            y_copy(ntile - 1).wait()

    def step(r, _):
        @pl.when(r < rounds)
        def _():
            def one(k, _):
                @pl.when(jnp.logical_and(k == per_round // 2 - 1, r > 0))
                def _():
                    fetch(r - 1)

                project(r * per_round + 2 * k, 0)
                project(r * per_round + 2 * k + 1, 1)
                return 0

            lax.fori_loop(0, per_round // 2, one, 0)

        @pl.when(r == rounds - 1)
        def _():
            turn(jnp.int32(tiles - 1), (tiles - 1) % 2)
            c_send(jnp.int32(tiles - 1))
            e_sent(jnp.int32(tiles - 1))

        @pl.when(jnp.logical_and(r > 2, end))
        def _():
            own_done(r - 3)

        @pl.when(r == rounds)
        def _():
            combine(0)
            fetch(r - 1)

        @pl.when(jnp.logical_and(r > 1, end))
        def _():
            own_fetch(r - 2)

        @pl.when(r > 0)
        def _():
            attend(r - 1)

        @pl.when(jnp.logical_and(r > 1, end))
        def _():
            own_attend(r - 2)

        return 0

    lax.fori_loop(0, rounds + 1, step, 0)
    own_sent(rounds - 1)

    @pl.when(end)
    def _():
        own_done(rounds - 2)
        own_fetch(rounds - 1)

    combine(1)

    @pl.when(end)
    def _():
        own_attend(rounds - 1)
        own_done(rounds - 1)

    combine(2)
    for i in range(tiles - SLOTS, tiles, 3):
        c_sent(jnp.int32(i))
    d_sent(rounds - 2)
    d_sent(rounds - 1)


def solution(mesh):
    n = mesh.shape["sp"]

    def step(x, gain, wq, wk, wv, wo):
        own, width = x.shape
        part = PER * HEAD
        rounds = width // (n * part)
        place = lax.axis_index("sp") * own + jnp.arange(own)
        half = HEAD // 2
        angle = place.astype(jnp.float32)[:, None] * THETA ** (-jnp.arange(half, dtype=jnp.float32) / half)
        cos, sin = jnp.cos(angle), jnp.sin(angle)
        one = jnp.ones((own, HEAD), jnp.float32)
        cos = jnp.stack([jnp.concatenate([cos, cos], -1), one])
        sin = jnp.stack([jnp.concatenate([-sin, sin], -1), 0 * one])
        anywhere, vmem = pl.BlockSpec(memory_space=pl.ANY), pl.BlockSpec(memory_space=pltpu.VMEM)
        y, *_ = pl.pallas_call(
            functools.partial(_kernel, n),
            out_shape=[jax.ShapeDtypeStruct((own, width), jnp.bfloat16),
                       jax.ShapeDtypeStruct((rounds, n, 3, own, part), jnp.bfloat16),
                       jax.ShapeDtypeStruct((own, width), jnp.bfloat16),
                       jax.ShapeDtypeStruct((rounds, n, 3, own, part), jnp.bfloat16),
                       jax.ShapeDtypeStruct((rounds, n, 8, own), jnp.float32)],
            in_specs=[anywhere, vmem, vmem, vmem] + [anywhere] * 4,
            out_specs=[anywhere] * 5,
            scratch_shapes=[
                pltpu.VMEM((own, width), jnp.bfloat16),
                pltpu.VMEM((2, width, TILE), jnp.bfloat16),
                pltpu.VMEM((width // TILE, own, TILE), jnp.float32),
                pltpu.VMEM((2, own, TILE), jnp.bfloat16),
                pltpu.VMEM((SLOTS // 3, TILE // part, 3, own, part), jnp.bfloat16),
                pltpu.VMEM((n, 3, own, part), jnp.bfloat16),
                pltpu.VMEM((PER, n, HEAD, own), jnp.bfloat16),
                pltpu.VMEM((2, n - 1, own, part), jnp.bfloat16),
                pltpu.VMEM((2, own, TILE), jnp.bfloat16),
                pltpu.VMEM((n, 3, own, part), jnp.bfloat16),
                pltpu.VMEM((n, own, part), jnp.bfloat16),
                pltpu.VMEM((n, 8, own), jnp.float32),
                pltpu.VMEM((2, 8, own), jnp.float32),
                pltpu.VMEM((2, PER, HEAD, own), jnp.float32),
                pltpu.VMEM((2, 8, own), jnp.float32),
                pltpu.SemaphoreType.DMA((1,)),
                pltpu.SemaphoreType.DMA((2,)),
                pltpu.SemaphoreType.DMA((SLOTS // 3, TILE // part)),
                pltpu.SemaphoreType.DMA((rounds, n)),
                pltpu.SemaphoreType.DMA((n,)),
                pltpu.SemaphoreType.DMA((2, n)),
                pltpu.SemaphoreType.DMA((rounds, n)),
                pltpu.SemaphoreType.DMA((2,)),
                pltpu.SemaphoreType.DMA((2,)),
                pltpu.SemaphoreType.DMA((SLOTS // 3, TILE // part)),
                pltpu.SemaphoreType.DMA((n,)),
                pltpu.SemaphoreType.DMA((n,)),
                pltpu.SemaphoreType.DMA((n,)),
                pltpu.SemaphoreType.DMA((n,)),
                pltpu.SemaphoreType.DMA((2,)),
                pltpu.SemaphoreType.DMA((rounds, n)),
            ],
            compiler_params=pltpu.CompilerParams(collective_id=0, has_side_effects=True, vmem_limit_bytes=67043328),
        )(x, gain[None], cos, sin, wq, wk, wv, wo)
        return y

    tokens, whole = P(("dp", "sp"), None), P(None, None)
    return jax.shard_map(
        step,
        mesh=mesh,
        in_specs=(tokens, P(None), whole, whole, whole, whole),
        out_specs=tokens,
        check_vma=False,
    )
```
